256 devices in a mesh: rows: 4 (over x_hi, core), vec: 64 (over y, x_lo, z).
Axes of the slice: x: 4 (x_hi: 2, x_lo: 2; x = x_hi * 2 + x_lo), y: 4, z: 8, core: 2. Of those that a mesh axis runs over, the one named last changes fastest.
Arguments:
- eigen_rows: float32 [2048, 8192], P('rows', 'vec'), may hold values from -6 to 6
- panels: float32 [3, 2048, 256], P(None, ('rows', 'vec')), may hold values from -0.25 to 0.25
Outputs:
- transformed: float32 [2048, 8192], P('rows', 'vec')
The draws below stay inside these ranges and needn't reach their ends.
All inputs are finite; a program needn't handle non-finite values.
Results may differ from the reference program's by a relative error of at most 0.00017.
Values sent between devices are 32-bit elements; how exact they have to be, the bound alone decides.
No kernel may reach another device: no remote copies, remote signals or barrier semaphores. Data moves between devices by JAX's collectives and lax.ppermute only.
A program may use at most 192 MiB of HBM per device.

```python
import jax
import jax.numpy as jnp
from jax import lax

REFLECTORS = 256
BLOCK_ROWS = 512
SLOTS = 3
ROWS = 2048
VECTORS = 8192


def block_scale(stream_key, shape, cuts, smallest, largest):
    gain, own = 1.0, jax.random.fold_in(stream_key, 6)
    for dim, blocks in cuts:
        steps = jnp.exp(jax.random.uniform(jax.random.fold_in(own, dim), (blocks,), jnp.float32, smallest / len(cuts), largest / len(cuts)))
        gain = gain * jnp.repeat(steps, shape[dim] // blocks).reshape([-1 if axis == dim else 1 for axis in range(len(shape))])
    return gain


def scatter_about(key, extent, scale, most, shards=(), held_as=jnp.bfloat16):
    array = jax.random.normal(key, extent, jnp.float32) * scale
    if len(shards) > 0:
        array = block_scale(key, extent, shards, -0.22, 0.18) * array
    return jnp.clip(array, min=-most, max=most).astype(held_as)


def setup_inputs(seed: int = 0) -> dict:
    streams_of = jax.random.split(jax.random.key(seed), 3)
    return {
        "eigen_rows": scatter_about(streams_of[0], (ROWS, VECTORS), 1.0, 6.0, ((0, 4), (1, 64)), jnp.float32),
        "panels": scatter_about(streams_of[1], (SLOTS, ROWS, REFLECTORS), BLOCK_ROWS ** -0.5, 0.25, ((1, 256),), jnp.float32),
    }


def reflect(panel_rows, values):
    block_len = panel_rows.shape[-2]
    width = panel_rows.shape[-1]
    shifted = panel_rows + jnp.eye(block_len, width, dtype=panel_rows.dtype)
    inner_products = jnp.einsum('...br,...bs->...rs', shifted, shifted, precision=lax.Precision.HIGHEST)
    triangle = jnp.triu(inner_products, 1) + 0.5 * inner_products * jnp.eye(width, dtype=panel_rows.dtype)
    projected = jnp.einsum('...br,...bc->...rc', shifted, values, precision=lax.Precision.HIGHEST)
    solved = jax.scipy.linalg.solve_triangular(triangle, projected, lower=False)
    return values - jnp.einsum('...br,...rc->...bc', shifted, solved, precision=lax.Precision.HIGHEST)

def reference(eigen_rows, panels):
    block_len = 2 * REFLECTORS
    columns = eigen_rows.shape[1]
    values = eigen_rows
    for sweep_set in range(SLOTS):
        offset = sweep_set % 2 * REFLECTORS
        pieces = (ROWS - 2 * offset) // block_len
        interior = values[offset:offset + pieces * block_len]
        panel_part = panels[sweep_set][offset:offset + pieces * block_len]
        applied = lax.map(lambda operands: reflect(operands[0], operands[1]), (panel_part.reshape(pieces, block_len, REFLECTORS), interior.reshape(pieces, block_len, columns)))
        applied = applied.reshape(pieces * block_len, columns)
        values = jnp.concatenate([values[:offset], applied, values[offset + pieces * block_len:]], axis=0)
    return values
```

```python
import jax
import jax.numpy as jnp
from jax import lax
from jax.experimental import pallas as pl
from jax.experimental.pallas import tpu as pltpu
from jax.sharding import Mesh, PartitionSpec as P

R = 256
H = 128
Q = 64
F32 = jnp.float32
BF16 = jnp.bfloat16


def halves(value):
    top = value.astype(BF16)
    return top, (value - top.astype(F32)).astype(BF16)


def dot(a, b):
    return jnp.dot(a, b, preferred_element_type=F32)


def product(a, b):
    return dot(a[0], b[0]) + (dot(a[0], b[1]) + dot(a[1], b[0]))


def exact(a, b):
    return jnp.dot(a, b, precision=lax.Precision.HIGHEST, preferred_element_type=F32)


def iota(shape, dim):
    return lax.broadcasted_iota(jnp.int32, shape, dim)


def with_eye(rows):
    return rows + (iota(rows.shape, 0) == iota(rows.shape, 1)).astype(F32)


def spread(tile, column):
    lanes = iota(tile.shape, 1)
    return jnp.take_along_axis(tile, (lanes & ~(Q - 1)) + column, axis=1)


def invert_unit(v00, v01, v11):
    low = iota((Q, H), 1) < Q
    out = []
    for v in (v00, v11):
        packed = jnp.where(low, v[:Q], v[Q:])
        strips = [packed[8 * i : 8 * i + 8] for i in range(Q // 8)]
        result = [
            ((iota((8, H), 1) & (Q - 1)) == iota((8, H), 0) + 8 * i).astype(F32)
            for i in range(Q // 8)
        ]
        for j in range(Q - 1, 0, -1):
            row = result[j // 8][j % 8 : j % 8 + 1]
            for i in range((j - 1) // 8 + 1):
                column = spread(strips[i], j)
                if i == j // 8:
                    column = jnp.where(iota((8, H), 0) < j % 8, column, 0.0)
                result[i] = result[i] - column * row
        packed = jnp.concatenate(result, axis=0)
        top = jnp.where(low, packed, 0.0)
        bottom = jnp.where(low, 0.0, packed)
        corner = jnp.where(low, 0.0, v[:Q])
        part = exact(corner, jnp.concatenate([top, bottom], axis=0))
        part = exact(top, jnp.concatenate([part, jnp.zeros_like(part)], axis=0))
        out.append(jnp.concatenate([top - part, bottom], axis=0))
    t00, t11 = out
    return t00, -exact(t00, exact(v01, t11)), t11


def inverse_of(g00, g01, g11, d00, d11):
    above = iota((H, H), 0) < iota((H, H), 1)
    eye = iota((H, H), 0) == iota((H, H), 1)
    r0, r1 = 2.0 / d00, 2.0 / d11
    v00 = jnp.where(above, g00 * r0, 0.0)
    v11 = jnp.where(above, g11 * r1, 0.0)
    t00, t01, t11 = invert_unit(v00, g01 * r1, v11)
    c0 = jnp.sum(jnp.where(eye, r0, 0.0), axis=1, keepdims=True)
    c1 = jnp.sum(jnp.where(eye, r1, 0.0), axis=1, keepdims=True)
    top = jnp.concatenate([t00 * c0, t01 * c0], axis=1)
    bottom = jnp.concatenate([jnp.zeros((H, H), F32), t11 * c1], axis=1)
    return jnp.concatenate([top, bottom], axis=0)


def diagonal(block):
    eye = iota((H, H), 0) == iota((H, H), 1)
    return jnp.sum(jnp.where(eye, block, 0.0), axis=0, keepdims=True)


def inverse_full(g):
    g00, g01, g11 = g[:H, :H], g[:H, H:], g[H:, H:]
    return inverse_of(g00, g01, g11, diagonal(g00), diagonal(g11))


def pack(g):
    keep = iota((H, H), 0) <= iota((H, H), 1)
    first = jnp.where(keep, g[:H, :H], g[H:, H:])
    diag = jnp.broadcast_to(diagonal(g[H:, H:]), (8, H))
    tail = jnp.concatenate([diag, jnp.zeros((8, H), F32)], axis=1)
    return jnp.concatenate([jnp.concatenate([first, g[:H, H:]], axis=1), tail], axis=0)


def inverse_packed(m, live):
    first, d11 = m[:H, :H], m[H : H + 1, :H]
    d00 = diagonal(first)
    one = jnp.where(live, 0.0, 1.0)
    return inverse_of(first, m[:H, H:], first.T, d00 + one, d11 + one)


def panel(ref, s):
    return ref[:, :, s].reshape(2 * R, R)


def gram_kernel(y_ref, low_ref, up_ref):
    rows = panel(y_ref, 1)
    for half, ref in ((with_eye(rows[R:]), low_ref), (rows[:R], up_ref)):
        ref[...] = pack(product(halves(half.T), halves(half)))


def first_kernel(y_ref, z_ref, out_ref, low_ref, up_ref):
    y = with_eye(panel(y_ref, 0))
    yh, yt = halves(y), halves(y.T)
    z = z_ref[...]
    p = product(yt, halves(z))
    t = inverse_full(product(yt, yh))
    x = product(halves(t), halves(p))
    z = z - product(yh, halves(x))
    out_ref[...] = z
    rows = panel(y_ref, 1)
    low_ref[...] = product(halves(with_eye(rows[R:]).T), halves(z[R:]))
    up_ref[...] = product(halves(rows[:R].T), halves(z[:R]))


def inverse_kernel(live_ref, low_ref, low_in_ref, up_ref, up_in_ref, y_ref, t_low_ref, t_up_ref, t_ref):
    t_low_ref[...] = inverse_packed(low_ref[...] + low_in_ref[...], live_ref[0] != 0)
    t_up_ref[...] = inverse_packed(up_ref[...] + up_in_ref[...], live_ref[1] != 0)
    y = with_eye(panel(y_ref, 2))
    t_ref[...] = inverse_full(product(halves(y.T), halves(y)))


def last_kernel(live_ref, y_ref, z_ref, low_ref, low_in_ref, up_ref, up_in_ref, t_low_ref, t_up_ref, t_ref, out_ref):
    rows = panel(y_ref, 1)
    z = z_ref[...]
    x_low = product(halves(t_low_ref[...]), halves(low_ref[...] + low_in_ref[...]))
    x_up = product(halves(t_up_ref[...]), halves(up_ref[...] + up_in_ref[...]))
    z_low = z[R:] - product(halves(with_eye(rows[R:])), halves(x_low))
    z_up = z[:R] - product(halves(rows[:R]), halves(x_up))
    z_low = jnp.where(live_ref[0] != 0, z_low, z[R:])
    z_up = jnp.where(live_ref[1] != 0, z_up, z[:R])
    z = jnp.concatenate([z_up, z_low], axis=0)
    y = with_eye(panel(y_ref, 2))
    p = product(halves(y.T), halves(z))
    x = product(halves(t_ref[...]), halves(p))
    out_ref[...] = z - product(halves(y), halves(x))


VM = pl.BlockSpec(memory_space=pltpu.VMEM)
SM = pl.BlockSpec(memory_space=pltpu.SMEM)


def call(kernel, outs, args, flops, scalars=0):
    return pl.pallas_call(
        kernel,
        out_shape=[jax.ShapeDtypeStruct(s, F32) for s in outs],
        in_specs=[SM] * scalars + [VM] * (len(args) - scalars),
        out_specs=[VM] * len(outs),
        cost_estimate=pl.CostEstimate(flops=flops, bytes_accessed=4 << 20, transcendentals=0),
        name=kernel.__name__,
    )(*args)


def copies(value, axes):
    count = lax.axis_size(axes)
    stack = jnp.broadcast_to(value, (count, *value.shape))
    return lax.all_to_all(stack, axes, split_axis=0, concat_axis=0, tiled=True)


def rows_shift(value, step):
    route = [(i, i + step) for i in range(4) if 0 <= i + step < 4]
    return lax.ppermute(value, ("xh", "core"), route)


def local(eigen_rows, panels):
    group = lax.axis_index("xh") * 2 + lax.axis_index("core")
    live = jnp.stack([group < 3, group > 0]).astype(jnp.int32)
    near = copies(panels, "z")
    y = copies(near, ("y", "xl"))
    y = y.reshape(8, 8, 3, 8, R)
    columns = eigen_rows.shape[1]
    big = 10**9
    low, up = call(gram_kernel, [(H + 8, R)] * 2, [y], big)
    low_in, up_in = rows_shift(up, -1), rows_shift(low, 1)
    z, p_low, p_up = call(
        first_kernel, [eigen_rows.shape, (R, columns), (R, columns)], [y, eigen_rows], 4 * big
    )
    p_low_in, p_up_in = rows_shift(p_up, -1), rows_shift(p_low, 1)
    ts = call(inverse_kernel, [(R, R)] * 3, [live, low, low_in, up, up_in, y], 4 * big, 1)
    (out,) = call(
        last_kernel,
        [eigen_rows.shape],
        [live, y, z, p_low, p_low_in, p_up, p_up_in, *ts],
        2 * big,
        1,
    )
    return out


def solution(mesh):
    fine = Mesh(mesh.devices.reshape(2, 2, 4, 2, 8), ("xh", "core", "y", "xl", "z"))
    slab = P(("xh", "core"), ("y", "xl", "z"))
    strips = P(None, ("xh", "core", "y", "xl", "z"), None)
    return jax.shard_map(local, mesh=fine, in_specs=(slab, strips), out_specs=slab, check_vma=False)
```

```python
import jax
import jax.numpy as jnp
from jax import lax
from jax.experimental import pallas as pl
from jax.experimental.pallas import tpu as pltpu
from jax.sharding import Mesh, PartitionSpec as P

R = 256
H = 128
Q = 32
F32 = jnp.float32
BF16 = jnp.bfloat16


def halves(value):
    top = value.astype(BF16)
    return top, (value - top.astype(F32)).astype(BF16)


def dot(a, b):
    return jnp.dot(a, b, preferred_element_type=F32)


def product(a, b):
    return dot(a[0], b[0]) + (dot(a[0], b[1]) + dot(a[1], b[0]))


def exact(a, b):
    return jnp.dot(a, b, precision=lax.Precision.HIGHEST, preferred_element_type=F32)


def iota(shape, dim):
    return lax.broadcasted_iota(jnp.int32, shape, dim)


def with_eye(rows):
    return rows + (iota(rows.shape, 0) == iota(rows.shape, 1)).astype(F32)


def spread(tile, column):
    lanes = iota(tile.shape, 1)
    return jnp.take_along_axis(tile, (lanes & ~(Q - 1)) + column, axis=1)


def invert_units(blocks):
    lanes, count = iota((8, H), 1), Q // 8
    strips, results = [], []
    for v in blocks:
        for i in range(count):
            strip = v[8 * i : 8 * i + 8]
            for k in range(1, H // Q):
                strip = jnp.where(lanes >= k * Q, v[k * Q + 8 * i : k * Q + 8 * i + 8], strip)
            strips.append(strip)
            results.append(((lanes & (Q - 1)) == iota((8, H), 0) + 8 * i).astype(F32))
    for j in range(Q - 1, 0, -1):
        for m in range(0, len(strips), count):
            row = results[m + j // 8][j % 8 : j % 8 + 1]
            for i in range((j - 1) // 8 + 1):
                column = spread(strips[m + i], j)
                if i == j // 8:
                    column = jnp.where(iota((8, H), 0) < j % 8, column, 0.0)
                results[m + i] = results[m + i] - column * row
    wide = iota((Q, H), 1)
    out = []
    for m in range(0, len(strips), count):
        packed = jnp.concatenate(results[m : m + count], axis=0)
        out.append(
            jnp.concatenate(
                [
                    jnp.where((wide >= k * Q) & (wide < (k + 1) * Q), packed, 0.0)
                    for k in range(H // Q)
                ],
                axis=0,
            )
        )
    span = Q
    rows, cols = iota((H, H), 0), iota((H, H), 1)
    while span < H:
        corner = ((rows & span) == 0) & ((cols & span) != 0)
        corner = corner & ((rows & ~(2 * span - 1)) == (cols & ~(2 * span - 1)))
        parts = [exact(t, jnp.where(corner, v, 0.0)) for t, v in zip(out, blocks)]
        out = [t - exact(part, t) for t, part in zip(out, parts)]
        span *= 2
    return out


def invert_unit_all(matrices):
    out = invert_units([v for v00, _, v11 in matrices for v in (v00, v11)])
    tops, bottoms = out[0::2], out[1::2]
    corners = [exact(v01, t11) for (_, v01, _), t11 in zip(matrices, bottoms)]
    corners = [-exact(t00, c) for t00, c in zip(tops, corners)]
    return list(zip(tops, corners, bottoms))


def inverses_of(grams):
    above = iota((H, H), 0) < iota((H, H), 1)
    eye = iota((H, H), 0) == iota((H, H), 1)
    units, scales = [], []
    for g00, g01, g11, d00, d11 in grams:
        r0, r1 = 2.0 / d00, 2.0 / d11
        units.append(
            (jnp.where(above, g00 * r0, 0.0), g01 * r1, jnp.where(above, g11 * r1, 0.0))
        )
        scales.append(
            [jnp.sum(jnp.where(eye, r, 0.0), axis=1, keepdims=True) for r in (r0, r1)]
        )
    out = []
    for (t00, t01, t11), (c0, c1) in zip(invert_unit_all(units), scales):
        top = jnp.concatenate([t00 * c0, t01 * c0], axis=1)
        bottom = jnp.concatenate([jnp.zeros((H, H), F32), t11 * c1], axis=1)
        out.append(jnp.concatenate([top, bottom], axis=0))
    return out


def diagonal(block):
    eye = iota((H, H), 0) == iota((H, H), 1)
    return jnp.sum(jnp.where(eye, block, 0.0), axis=0, keepdims=True)


def full_parts(g):
    g00, g01, g11 = g[:H, :H], g[:H, H:], g[H:, H:]
    return g00, g01, g11, diagonal(g00), diagonal(g11)


def pack(g):
    keep = iota((H, H), 0) <= iota((H, H), 1)
    first = jnp.where(keep, g[:H, :H], g[H:, H:])
    diag = jnp.broadcast_to(diagonal(g[H:, H:]), (8, H))
    tail = jnp.concatenate([diag, jnp.zeros((8, H), F32)], axis=1)
    return jnp.concatenate([jnp.concatenate([first, g[:H, H:]], axis=1), tail], axis=0)


def packed_parts(m, live):
    first, d11 = m[:H, :H], m[H : H + 1, :H]
    one = jnp.where(live, 0.0, 1.0)
    return first, m[:H, H:], first.T, diagonal(first) + one, d11 + one


def panel(ref, s):
    return ref[:, :, s].reshape(2 * R, R)


def spread_kernel(value_ref, out_ref):
    for i in range(out_ref.shape[0]):
        out_ref[i] = value_ref[...]


def spread_parts_kernel(value_ref, *outs):
    start = 0
    for out_ref in outs:
        stop = start + out_ref.shape[2]
        for i in range(out_ref.shape[0]):
            out_ref[i] = value_ref[:, start:stop]
        start = stop


def gram_kernel(core_ref, g_ref, c_ref, x_ref, yh_ref, yl_ref, th_ref, tl_ref):
    rows = panel(g_ref, 1)
    packed = []
    for k, half in enumerate((rows[:R], with_eye(rows[R:]))):
        y, t = halves(half), halves(half.T)
        packed.append(pack(product(t, y)))
        yh_ref[k], yl_ref[k] = y
        th_ref[k], tl_ref[k] = t
    up, low = packed
    first = core_ref[0] == 0
    c_ref[...] = jnp.where(first, low, up)
    x_ref[...] = jnp.where(first, up, low)


def first_kernel(core_ref, g_ref, z_ref, th_ref, tl_ref, out_ref, c_ref, x_ref):
    y = with_eye(panel(g_ref, 0))
    yh, yt = halves(y), halves(y.T)
    z = z_ref[...]
    p = product(yt, halves(z))
    (t,) = inverses_of([full_parts(product(yt, yh))])
    x = exact(t, p)
    z = z - product(yh, halves(x))
    up = product((th_ref[0], tl_ref[0]), halves(z[:R]))
    low = product((th_ref[1], tl_ref[1]), halves(z[R:]))
    first = core_ref[0] == 0
    c_ref[...] = jnp.where(first, low, up)
    x_ref[...] = jnp.where(first, up, low)
    out_ref[...] = z


def second_kernel(core_ref, g_ref, c_ref, c_in_ref, x_ref, x_in_ref, th_ref, tl_ref, t_ref, tc_ref, tx_ref):
    y = with_eye(panel(g_ref, 0))
    yh, yt = halves(y), halves(y.T)
    th_ref[...], tl_ref[...] = yt
    t_ref[...], tc_ref[...], tx_ref[...] = inverses_of(
        [
            full_parts(product(yt, yh)),
            packed_parts(c_ref[...] + c_in_ref[...], True),
            packed_parts(x_ref[...] + x_in_ref[...], core_ref[1] != 0),
        ]
    )


def last_kernel(core_ref, g_ref, z_ref, c_ref, c_in_ref, x_ref, x_in_ref, tc_ref, tx_ref,
                ah_ref, al_ref, th_ref, tl_ref, t_ref, out_ref):
    xc = exact(tc_ref[...], c_ref[...] + c_in_ref[...])
    xx = exact(tx_ref[...], x_ref[...] + x_in_ref[...])
    xx = jnp.where(core_ref[1] != 0, xx, 0.0)
    first = core_ref[0] == 0
    z_up = z_ref[:R] - product((ah_ref[0], al_ref[0]), halves(jnp.where(first, xx, xc)))
    z_low = z_ref[R:] - product((ah_ref[1], al_ref[1]), halves(jnp.where(first, xc, xx)))
    z = jnp.concatenate([z_up, z_low], axis=0)
    p = product((th_ref[...], tl_ref[...]), halves(z))
    x = exact(t_ref[...], p)
    out_ref[...] = z - product(halves(with_eye(panel(g_ref, 0))), halves(x))


VM = pl.BlockSpec(memory_space=pltpu.VMEM)
SM = pl.BlockSpec(memory_space=pltpu.SMEM)


def call(kernel, outs, args, flops, scalars=0):
    outs = [o if isinstance(o[0], tuple) else (o, F32) for o in outs]
    return pl.pallas_call(
        kernel,
        out_shape=[jax.ShapeDtypeStruct(s, d) for s, d in outs],
        in_specs=[SM] * scalars + [VM] * (len(args) - scalars),
        out_specs=[VM] * len(outs),
        cost_estimate=pl.CostEstimate(flops=flops, bytes_accessed=1 << 20, transcendentals=0),
        compiler_params=pltpu.CompilerParams(vmem_limit_bytes=12 << 20),
        name=kernel.__name__,
    )(*args)


def exchange(stack, axes):
    return lax.all_to_all(stack, axes, split_axis=0, concat_axis=0, tiled=True)


def swap_cores(value):
    return lax.ppermute(value, "core", [(0, 1), (1, 0)])


def swap_middle(value):
    return lax.ppermute(value, ("xh", "core"), [(1, 2), (2, 1)])


def local(eigen_rows, panels):
    core = lax.axis_index("core")
    group = lax.axis_index("xh") * 2 + core
    flags = jnp.stack([core, (group == 1) | (group == 2)]).astype(jnp.int32)
    (stack,) = call(spread_kernel, [(8, *panels.shape)], [panels], 10**6)
    near = exchange(stack, "z")
    early, late = call(
        spread_parts_kernel, [(8, 8, 2, 8, R), (8, 8, 1, 8, R)], [near], 10**6
    )
    every = exchange(early, ("y", "xl"))
    third = exchange(late, ("y", "xl"))
    columns = eigen_rows.shape[1]
    half = ((2, R, R), BF16)
    big = 10**9
    c, x, ah, al, bh, bl = call(
        gram_kernel, [(H + 8, R)] * 2 + [half] * 4, [flags, every], big, 1
    )
    x_in, c_in = swap_middle(x), swap_cores(c)
    z, pc, px = call(
        first_kernel,
        [eigen_rows.shape, (R, columns), (R, columns)],
        [flags, every, eigen_rows, bh, bl],
        8 * big,
        1,
    )
    px_in, pc_in = swap_middle(px), swap_cores(pc)
    th, tl, t, tc, tx = call(
        second_kernel,
        [((R, 2 * R), BF16)] * 2 + [(R, R)] * 3,
        [flags, third, c, c_in, x, x_in],
        8 * big,
        1,
    )
    (out,) = call(
        last_kernel,
        [eigen_rows.shape],
        [flags, third, z, pc, pc_in, px, px_in, tc, tx, ah, al, th, tl, t],
        2 * big,
        1,
    )
    return out


def solution(mesh):
    fine = Mesh(mesh.devices.reshape(2, 2, 4, 2, 8), ("xh", "core", "y", "xl", "z"))
    slab = P(("xh", "core"), ("y", "xl", "z"))
    strips = P(None, ("xh", "core", "y", "xl", "z"), None)
    return jax.shard_map(local, mesh=fine, in_specs=(slab, strips), out_specs=slab, check_vma=False)
```

```python
import jax
import jax.numpy as jnp
from jax import lax
from jax.experimental import pallas as pl
from jax.experimental.pallas import tpu as pltpu
from jax.sharding import Mesh, PartitionSpec as P

R = 256
H = 128
Q = 32
F32 = jnp.float32
BF16 = jnp.bfloat16


def halves(value):
    top = value.astype(BF16)
    return top, (value - top.astype(F32)).astype(BF16)


def dot(a, b):
    return jnp.dot(a, b, preferred_element_type=F32)


def product(a, b):
    return dot(a[0], b[0]) + (dot(a[0], b[1]) + dot(a[1], b[0]))


def exact(a, b):
    return jnp.dot(a, b, precision=lax.Precision.HIGHEST, preferred_element_type=F32)


def iota(shape, dim):
    return lax.broadcasted_iota(jnp.int32, shape, dim)


def with_eye(rows):
    return rows + (iota(rows.shape, 0) == iota(rows.shape, 1)).astype(F32)


def spread(tile, column):
    lanes = iota(tile.shape, 1)
    return jnp.take_along_axis(tile, (lanes & ~(Q - 1)) + column, axis=1)


def invert_units(blocks):
    lanes, count = iota((8, H), 1), Q // 8
    strips, results = [], []
    for v in blocks:
        for i in range(count):
            strip = v[8 * i : 8 * i + 8]
            for k in range(1, H // Q):
                strip = jnp.where(lanes >= k * Q, v[k * Q + 8 * i : k * Q + 8 * i + 8], strip)
            strips.append(strip)
            results.append(((lanes & (Q - 1)) == iota((8, H), 0) + 8 * i).astype(F32))
    for j in range(Q - 1, 0, -1):
        for m in range(0, len(strips), count):
            row = results[m + j // 8][j % 8 : j % 8 + 1]
            for i in range((j - 1) // 8 + 1):
                column = spread(strips[m + i], j)
                if i == j // 8:
                    column = jnp.where(iota((8, H), 0) < j % 8, column, 0.0)
                results[m + i] = results[m + i] - column * row
    wide = iota((Q, H), 1)
    out = []
    for m in range(0, len(strips), count):
        packed = jnp.concatenate(results[m : m + count], axis=0)
        out.append(
            jnp.concatenate(
                [
                    jnp.where((wide >= k * Q) & (wide < (k + 1) * Q), packed, 0.0)
                    for k in range(H // Q)
                ],
                axis=0,
            )
        )
    span = Q
    while span < H:
        starts = range(0, H, 2 * span)

        def chosen(value):
            return jnp.concatenate([value[i : i + span] for i in starts], axis=0)

        def placed(value):
            gap, strips = jnp.zeros((span, H), F32), []
            for i in range(len(starts)):
                strips += [value[i * span : (i + 1) * span], gap]
            return jnp.concatenate(strips, axis=0)

        rows, cols = iota((H // 2, H), 0), iota((H // 2, H), 1)
        corner = ((cols & span) != 0) & (rows // span == cols // (2 * span))
        parts = [exact(jnp.where(corner, chosen(v), 0.0), t) for t, v in zip(out, blocks)]
        parts = [exact(chosen(t), placed(part)) for t, part in zip(out, parts)]
        out = [t - placed(part) for t, part in zip(out, parts)]
        span *= 2
    return out


def invert_unit_all(matrices):
    out = invert_units([v for v00, _, v11 in matrices for v in (v00, v11)])
    tops, bottoms = out[0::2], out[1::2]
    corners = [exact(v01, t11) for (_, v01, _), t11 in zip(matrices, bottoms)]
    corners = [-exact(t00, c) for t00, c in zip(tops, corners)]
    return list(zip(tops, corners, bottoms))


def inverses_of(grams):
    above = iota((H, H), 0) < iota((H, H), 1)
    eye = iota((H, H), 0) == iota((H, H), 1)
    units, scales = [], []
    for g00, g01, g11, d00, d11 in grams:
        r0, r1 = 2.0 / d00, 2.0 / d11
        units.append(
            (jnp.where(above, g00 * r0, 0.0), g01 * r1, jnp.where(above, g11 * r1, 0.0))
        )
        scales.append(
            [jnp.sum(jnp.where(eye, r, 0.0), axis=1, keepdims=True) for r in (r0, r1)]
        )
    out = []
    for (t00, t01, t11), (c0, c1) in zip(invert_unit_all(units), scales):
        top = jnp.concatenate([t00 * c0, t01 * c0], axis=1)
        bottom = jnp.concatenate([jnp.zeros((H, H), F32), t11 * c1], axis=1)
        out.append(jnp.concatenate([top, bottom], axis=0))
    return out


def diagonal(block):
    eye = iota((H, H), 0) == iota((H, H), 1)
    return jnp.sum(jnp.where(eye, block, 0.0), axis=0, keepdims=True)


def full_parts(g):
    g00, g01, g11 = g[:H, :H], g[:H, H:], g[H:, H:]
    return g00, g01, g11, diagonal(g00), diagonal(g11)


def pack(g):
    keep = iota((H, H), 0) <= iota((H, H), 1)
    first = jnp.where(keep, g[:H, :H], g[H:, H:])
    diag = jnp.broadcast_to(diagonal(g[H:, H:]), (8, H))
    tail = jnp.concatenate([diag, jnp.zeros((8, H), F32)], axis=1)
    return jnp.concatenate([jnp.concatenate([first, g[:H, H:]], axis=1), tail], axis=0)


def packed_parts(m, live):
    first, d11 = m[:H, :H], m[H : H + 1, :H]
    one = jnp.where(live, 0.0, 1.0)
    return first, m[:H, H:], first.T, diagonal(first) + one, d11 + one


def panel(ref, s):
    return ref[:, :, s].reshape(2 * R, R)


def spread_kernel(value_ref, out_ref):
    for i in range(out_ref.shape[0]):
        out_ref[i] = value_ref[...]


def spread_parts_kernel(value_ref, *outs):
    start = 0
    for out_ref in outs:
        stop = start + out_ref.shape[2]
        for i in range(out_ref.shape[0]):
            out_ref[i] = value_ref[:, start:stop]
        start = stop


def first_kernel(core_ref, g_ref, z_ref, out_ref, pc_ref, px_ref, c_ref, x_ref, ah_ref, al_ref):
    first = core_ref[0] == 0
    rows = panel(g_ref, 1)
    packed, turned = [], []
    for k, half in enumerate((rows[:R], with_eye(rows[R:]))):
        y, t = halves(half), halves(half.T)
        packed.append(pack(product(t, y)))
        turned.append(t)
        ah_ref[k], al_ref[k] = y
    up, low = packed
    c_ref[...] = jnp.where(first, low, up)
    x_ref[...] = jnp.where(first, up, low)
    y = with_eye(panel(g_ref, 0))
    yh, yt = halves(y), halves(y.T)
    z = z_ref[...]
    p = product(yt, halves(z))
    (t,) = inverses_of([full_parts(product(yt, yh))])
    x = exact(t, p)
    z = z - product(yh, halves(x))
    out_ref[...] = z
    up = product(turned[0], halves(z[:R]))
    low = product(turned[1], halves(z[R:]))
    pc_ref[...] = jnp.where(first, low, up)
    px_ref[...] = jnp.where(first, up, low)


def third_kernel(g_ref, th_ref, tl_ref, t_ref):
    y = with_eye(panel(g_ref, 0))
    yh, yt = halves(y), halves(y.T)
    th_ref[...], tl_ref[...] = yt
    (t_ref[...],) = inverses_of([full_parts(product(yt, yh))])


def second_kernel(core_ref, c_ref, c_in_ref, x_ref, x_in_ref, tc_ref, tx_ref):
    tc_ref[...], tx_ref[...] = inverses_of(
        [
            packed_parts(c_ref[...] + c_in_ref[...], True),
            packed_parts(x_ref[...] + x_in_ref[...], core_ref[1] != 0),
        ]
    )


def last_kernel(core_ref, g_ref, z_ref, c_ref, c_in_ref, x_ref, x_in_ref, tc_ref, tx_ref,
                ah_ref, al_ref, th_ref, tl_ref, t_ref, out_ref):
    xc = exact(tc_ref[...], c_ref[...] + c_in_ref[...])
    xx = exact(tx_ref[...], x_ref[...] + x_in_ref[...])
    xx = jnp.where(core_ref[1] != 0, xx, 0.0)
    first = core_ref[0] == 0
    z_up = z_ref[:R] - product((ah_ref[0], al_ref[0]), halves(jnp.where(first, xx, xc)))
    z_low = z_ref[R:] - product((ah_ref[1], al_ref[1]), halves(jnp.where(first, xc, xx)))
    z = jnp.concatenate([z_up, z_low], axis=0)
    p = product((th_ref[...], tl_ref[...]), halves(z))
    x = exact(t_ref[...], p)
    out_ref[...] = z - product(halves(with_eye(panel(g_ref, 0))), halves(x))


VM = pl.BlockSpec(memory_space=pltpu.VMEM)
SM = pl.BlockSpec(memory_space=pltpu.SMEM)


def call(kernel, outs, args, flops, scalars=0):
    outs = [o if isinstance(o[0], tuple) else (o, F32) for o in outs]
    return pl.pallas_call(
        kernel,
        out_shape=[jax.ShapeDtypeStruct(s, d) for s, d in outs],
        in_specs=[SM] * scalars + [VM] * (len(args) - scalars),
        out_specs=[VM] * len(outs),
        cost_estimate=pl.CostEstimate(flops=flops, bytes_accessed=1 << 20, transcendentals=0),
        compiler_params=pltpu.CompilerParams(vmem_limit_bytes=12 << 20),
    )(*args)


def exchange(stack, axes):
    return lax.all_to_all(stack, axes, split_axis=0, concat_axis=0, tiled=True)


def swap_cores(value):
    return lax.ppermute(value, "core", [(0, 1), (1, 0)])


def swap_middle(value):
    return lax.ppermute(value, ("xh", "core"), [(1, 2), (2, 1)])


def local(eigen_rows, panels):
    core = lax.axis_index("core")
    group = lax.axis_index("xh") * 2 + core
    flags = jnp.stack([core, (group == 1) | (group == 2)]).astype(jnp.int32)
    panels, flags = lax.optimization_barrier((panels, flags))
    (stack,) = call(spread_kernel, [(8, *panels.shape)], [panels], 10**6)
    near = exchange(stack, "z")
    early, late = call(
        spread_parts_kernel, [(8, 8, 2, 8, R), (8, 8, 1, 8, R)], [near], 10**6
    )
    every = exchange(early, ("y", "xl"))
    third = exchange(late, ("y", "xl"))
    columns = eigen_rows.shape[1]
    half = ((2, R, R), BF16)
    big = 10**9
    z, pc, px, c, x, ah, al = call(
        first_kernel,
        [eigen_rows.shape, (R, columns), (R, columns)] + [(H + 8, R)] * 2 + [half] * 2,
        [flags, every, eigen_rows],
        8 * big,
        1,
    )
    x_in, c_in = swap_middle(x), swap_cores(c)
    px_in, pc_in = swap_middle(px), swap_cores(pc)
    th, tl, t = call(third_kernel, [((R, 2 * R), BF16)] * 2 + [(R, R)], [third], 4 * big)
    tc, tx = call(second_kernel, [(R, R)] * 2, [flags, c, c_in, x, x_in], 4 * big, 1)
    (out,) = call(
        last_kernel,
        [eigen_rows.shape],
        [flags, third, z, pc, pc_in, px, px_in, tc, tx, ah, al, th, tl, t],
        2 * big,
        1,
    )
    return out


def solution(mesh):
    fine = Mesh(mesh.devices.reshape(2, 2, 4, 2, 8), ("xh", "core", "y", "xl", "z"))
    slab = P(("xh", "core"), ("y", "xl", "z"))
    strips = P(None, ("xh", "core", "y", "xl", "z"), None)
    return jax.shard_map(local, mesh=fine, in_specs=(slab, strips), out_specs=slab, check_vma=False)
```

```python
import jax
import jax.numpy as jnp
from jax import lax
from jax.experimental import pallas as pl
from jax.experimental.pallas import tpu as pltpu
from jax.sharding import Mesh, PartitionSpec as P

R = 256
H = 128
Q = 32
F32 = jnp.float32
BF16 = jnp.bfloat16


def halves(value):
    top = value.astype(BF16)
    return top, (value - top.astype(F32)).astype(BF16)


def dot(a, b):
    return jnp.dot(a, b, preferred_element_type=F32)


def product(a, b):
    if b[0].shape[1] > H:
        return dot(a[0], b[0]) + (dot(a[0], b[1]) + dot(a[1], b[0]))
    both = dot(a[0], jnp.concatenate(b, axis=1))
    return both[:, :H] + (both[:, H:] + dot(a[1], b[0]))


def thirds(value):
    top = value.astype(BF16)
    rest = value - top.astype(F32)
    middle = rest.astype(BF16)
    return top, middle, (rest - middle.astype(F32)).astype(BF16)


def exact(a, b):
    a0, a1, a2 = thirds(a)
    b0, b1, b2 = thirds(b)
    small = dot(jnp.concatenate([a0, a2], axis=1), jnp.concatenate([b2, b0], axis=0))
    pair = jnp.concatenate([b0, b1], axis=1)
    if a.shape[1] > H:
        first, second = dot(a0, pair), dot(a1, pair)
        cross = first[:, H:] + second[:, :H]
        return first[:, :H] + (cross + (second[:, H:] + small))
    swapped = jnp.concatenate([b1, b0], axis=1)
    both = dot(jnp.concatenate([a0, a1], axis=1), jnp.concatenate([pair, swapped], axis=0))
    return both[:, :H] + (both[:, H:] + small)


def iota(shape, dim):
    return lax.broadcasted_iota(jnp.int32, shape, dim)


def with_eye(rows):
    return rows + (iota(rows.shape, 0) == iota(rows.shape, 1)).astype(F32)


def spread(tile, column):
    lanes = iota(tile.shape, 1)
    return jnp.take_along_axis(tile, (lanes & ~(Q - 1)) + column, axis=1)


def invert_units(blocks):
    lanes, count = iota((8, H), 1), Q // 8
    strips, results = [], []
    for v in blocks:
        for i in range(count):
            strip = v[8 * i : 8 * i + 8]
            for k in range(1, H // Q):
                strip = jnp.where(lanes >= k * Q, v[k * Q + 8 * i : k * Q + 8 * i + 8], strip)
            strips.append(strip)
            results.append(((lanes & (Q - 1)) == iota((8, H), 0) + 8 * i).astype(F32))
    for j in range(Q - 1, 0, -1):
        for m in range(0, len(strips), count):
            row = results[m + j // 8][j % 8 : j % 8 + 1]
            for i in range((j - 1) // 8 + 1):
                column = spread(strips[m + i], j)
                if i == j // 8:
                    column = jnp.where(iota((8, H), 0) < j % 8, column, 0.0)
                results[m + i] = results[m + i] - column * row
    wide = iota((Q, H), 1)
    out = []
    for m in range(0, len(strips), count):
        packed = jnp.concatenate(results[m : m + count], axis=0)
        out.append(
            jnp.concatenate(
                [
                    jnp.where((wide >= k * Q) & (wide < (k + 1) * Q), packed, 0.0)
                    for k in range(H // Q)
                ],
                axis=0,
            )
        )
    span = Q
    while span < H:
        starts = range(0, H, 2 * span)

        def chosen(value):
            return jnp.concatenate([value[i : i + span] for i in starts], axis=0)

        def placed(value):
            gap, strips = jnp.zeros((span, H), F32), []
            for i in range(len(starts)):
                strips += [value[i * span : (i + 1) * span], gap]
            return jnp.concatenate(strips, axis=0)

        rows, cols = iota((H // 2, H), 0), iota((H // 2, H), 1)
        corner = ((cols & span) != 0) & (rows // span == cols // (2 * span))
        parts = [exact(jnp.where(corner, chosen(v), 0.0), t) for t, v in zip(out, blocks)]
        parts = [exact(chosen(t), placed(part)) for t, part in zip(out, parts)]
        out = [t - placed(part) for t, part in zip(out, parts)]
        span *= 2
    return out


def invert_unit_all(matrices):
    out = invert_units([v for v00, _, v11 in matrices for v in (v00, v11)])
    tops, bottoms = out[0::2], out[1::2]
    corners = [exact(v01, t11) for (_, v01, _), t11 in zip(matrices, bottoms)]
    corners = [-exact(t00, c) for t00, c in zip(tops, corners)]
    return list(zip(tops, corners, bottoms))


def scaled(parts):
    g00, g01, g11, d00, d11 = parts
    above = iota((H, H), 0) < iota((H, H), 1)
    eye = iota((H, H), 0) == iota((H, H), 1)
    r0, r1 = 2.0 / d00, 2.0 / d11
    unit = jnp.where(above, g00 * r0, 0.0), g01 * r1, jnp.where(above, g11 * r1, 0.0)
    scale = [jnp.sum(jnp.where(eye, r, 0.0), axis=1, keepdims=True) for r in (r0, r1)]
    return unit, scale


def solve(parts, p):
    (v00, v01, v11), (c0, c1) = scaled(parts)
    t00, t11 = invert_units([v00, v11])
    x1 = exact(t11, p[H:])
    x0 = exact(t00, p[:H] - exact(v01, x1))
    return jnp.concatenate([x0 * c0, x1 * c1], axis=0)


def inverses_of(grams):
    units, scales = zip(*[scaled(parts) for parts in grams])
    out = []
    for (t00, t01, t11), (c0, c1) in zip(invert_unit_all(units), scales):
        top = jnp.concatenate([t00 * c0, t01 * c0], axis=1)
        bottom = jnp.concatenate([jnp.zeros((H, H), F32), t11 * c1], axis=1)
        out.append(jnp.concatenate([top, bottom], axis=0))
    return out


def diagonal(block):
    eye = iota((H, H), 0) == iota((H, H), 1)
    return jnp.sum(jnp.where(eye, block, 0.0), axis=0, keepdims=True)


def full_parts(g):
    g00, g01, g11 = g[:H, :H], g[:H, H:], g[H:, H:]
    return g00, g01, g11, diagonal(g00), diagonal(g11)


def pack(g):
    keep = iota((H, H), 0) <= iota((H, H), 1)
    first = jnp.where(keep, g[:H, :H], g[H:, H:])
    diag = jnp.broadcast_to(diagonal(g[H:, H:]), (8, H))
    tail = jnp.concatenate([diag, jnp.zeros((8, H), F32)], axis=1)
    return jnp.concatenate([jnp.concatenate([first, g[:H, H:]], axis=1), tail], axis=0)


def packed_parts(m, live):
    first, d11 = m[:H, :H], m[H : H + 1, :H]
    one = jnp.where(live, 0.0, 1.0)
    return first, m[:H, H:], first.T, diagonal(first) + one, d11 + one


def panel(ref, s):
    return ref[:, :, s].reshape(2 * R, R)


def spread_kernel(value_ref, out_ref):
    for i in range(out_ref.shape[0]):
        out_ref[i] = value_ref[...]


def spread_parts_kernel(value_ref, *outs):
    start = 0
    for out_ref in outs:
        stop = start + out_ref.shape[2]
        for i in range(out_ref.shape[0]):
            out_ref[i] = value_ref[:, start:stop]
        start = stop


def in_middle():
    return lax.axis_index("xh") != lax.axis_index("core")


def store_by_core(core, low, up, c_ref, x_ref):
    @pl.when(core == 0)
    def _():
        c_ref[...] = low
        x_ref[...] = up

    @pl.when(core != 0)
    def _():
        c_ref[...] = up
        x_ref[...] = low


def first_kernel(g_ref, z_ref, out_ref, pc_ref, px_ref, c_ref, x_ref, ah_ref, al_ref):
    rows = panel(g_ref, 1)
    packed, turned = [], []
    for k, half in enumerate((rows[:R], with_eye(rows[R:]))):
        y, t = halves(half), halves(half.T)
        packed.append(pack(product(t, y)))
        turned.append(t)
        ah_ref[k], al_ref[k] = y
    y = with_eye(panel(g_ref, 0))
    yh, yt = halves(y), halves(y.T)
    z = z_ref[...]
    p = product(yt, halves(z))
    x = solve(full_parts(product(yt, yh)), p)
    z = z - product(yh, halves(x))
    out_ref[...] = z
    up = product(turned[0], halves(z[:R]))
    low = product(turned[1], halves(z[R:]))
    store_by_core(lax.axis_index("core"), low, up, pc_ref, px_ref)
    store_by_core(lax.axis_index("core"), packed[1], packed[0], c_ref, x_ref)


def second_kernel(g_ref, c_ref, c_in_ref, x_ref, x_in_ref, th_ref, tl_ref, t_ref, tc_ref, tx_ref):
    y = with_eye(panel(g_ref, 0))
    yh, yt = halves(y), halves(y.T)
    th_ref[...], tl_ref[...] = yt
    t_ref[...], tc_ref[...], tx_ref[...] = inverses_of(
        [
            full_parts(product(yt, yh)),
            packed_parts(c_ref[...] + c_in_ref[...], True),
            packed_parts(x_ref[...] + x_in_ref[...], in_middle()),
        ]
    )


def last_kernel(g_ref, z_ref, c_ref, c_in_ref, x_ref, x_in_ref, tc_ref, tx_ref,
                ah_ref, al_ref, th_ref, tl_ref, t_ref, out_ref):
    xc = exact(tc_ref[...], c_ref[...] + c_in_ref[...])
    xx = exact(tx_ref[...], x_ref[...] + x_in_ref[...])
    xx = jnp.where(in_middle(), xx, 0.0)
    for half, x in ((1 - lax.axis_index("core"), xc), (lax.axis_index("core"), xx)):
        rows = pl.ds(pl.multiple_of(half * R, R), R)
        out_ref[rows, :] = z_ref[rows, :] - product((ah_ref[half], al_ref[half]), halves(x))
    z = out_ref[...]
    p = product((th_ref[...], tl_ref[...]), halves(z))
    x = exact(t_ref[...], p)
    out_ref[...] = z - product(halves(with_eye(panel(g_ref, 0))), halves(x))


VM = pl.BlockSpec(memory_space=pltpu.VMEM)
SM = pl.BlockSpec(memory_space=pltpu.SMEM)


def call(kernel, outs, args, flops, scalars=0):
    outs = [o if isinstance(o[0], tuple) else (o, F32) for o in outs]
    return pl.pallas_call(
        kernel,
        out_shape=[jax.ShapeDtypeStruct(s, d) for s, d in outs],
        in_specs=[SM] * scalars + [VM] * (len(args) - scalars),
        out_specs=[VM] * len(outs),
        cost_estimate=pl.CostEstimate(flops=flops, bytes_accessed=1 << 20, transcendentals=0),
        compiler_params=pltpu.CompilerParams(vmem_limit_bytes=12 << 20),
    )(*args)


def exchange(stack, axes):
    return lax.all_to_all(stack, axes, split_axis=0, concat_axis=0, tiled=True)


def swap_cores(value):
    return lax.ppermute(value, "core", [(0, 1), (1, 0)])


def swap_middle(value):
    return lax.ppermute(value, ("xh", "core"), [(1, 2), (2, 1)])


def local(eigen_rows, panels):
    (stack,) = call(spread_kernel, [(8, *panels.shape)], [panels], 10**6)
    near = exchange(stack, "z")
    early, late = call(
        spread_parts_kernel, [(8, 8, 2, 8, R), (8, 8, 1, 8, R)], [near], 10**6
    )
    every = exchange(early, ("y", "xl"))
    third = exchange(late, ("y", "xl"))
    columns = eigen_rows.shape[1]
    half = ((2, R, R), BF16)
    big = 10**9
    z, pc, px, c, x, ah, al = call(
        first_kernel,
        [eigen_rows.shape, (R, columns), (R, columns)] + [(H + 8, R)] * 2 + [half] * 2,
        [every, eigen_rows],
        8 * big,
    )
    x_in, c_in = swap_middle(x), swap_cores(c)
    px_in, pc_in = swap_middle(px), swap_cores(pc)
    th, tl, t, tc, tx = call(
        second_kernel,
        [((R, 2 * R), BF16)] * 2 + [(R, R)] * 3,
        [third, c, c_in, x, x_in],
        8 * big,
    )
    (out,) = call(
        last_kernel,
        [eigen_rows.shape],
        [third, z, pc, pc_in, px, px_in, tc, tx, ah, al, th, tl, t],
        2 * big,
    )
    return out


def solution(mesh):
    fine = Mesh(mesh.devices.reshape(2, 2, 4, 2, 8), ("xh", "core", "y", "xl", "z"))
    slab = P(("xh", "core"), ("y", "xl", "z"))
    strips = P(None, ("xh", "core", "y", "xl", "z"), None)
    return jax.shard_map(local, mesh=fine, in_specs=(slab, strips), out_specs=slab, check_vma=False)
```

```python
import jax
import jax.numpy as jnp
from jax import lax
from jax.experimental import pallas as pl
from jax.experimental.pallas import tpu as pltpu
from jax.sharding import Mesh, PartitionSpec as P

R = 256
H = 128
Q = 16
F32 = jnp.float32
BF16 = jnp.bfloat16


def halves(value):
    top = value.astype(BF16)
    return top, (value - top.astype(F32)).astype(BF16)


def dot(a, b):
    return jnp.dot(a, b, preferred_element_type=F32)


def product(a, b):
    if b[0].shape[1] > H:
        return dot(a[0], b[0]) + (dot(a[0], b[1]) + dot(a[1], b[0]))
    both = dot(a[0], jnp.concatenate(b, axis=1))
    return both[:, :H] + (both[:, H:] + dot(a[1], b[0]))


def thirds(value):
    top = value.astype(BF16)
    rest = value - top.astype(F32)
    middle = rest.astype(BF16)
    return top, middle, (rest - middle.astype(F32)).astype(BF16)


def exact(a, b):
    a0, a1, a2 = thirds(a)
    b0, b1, b2 = thirds(b)
    small = dot(jnp.concatenate([a0, a2], axis=1), jnp.concatenate([b2, b0], axis=0))
    pair = jnp.concatenate([b0, b1], axis=1)
    if a.shape[1] > H:
        first, second = dot(a0, pair), dot(a1, pair)
        cross = first[:, H:] + second[:, :H]
        return first[:, :H] + (cross + (second[:, H:] + small))
    swapped = jnp.concatenate([b1, b0], axis=1)
    both = dot(jnp.concatenate([a0, a1], axis=1), jnp.concatenate([pair, swapped], axis=0))
    return both[:, :H] + (both[:, H:] + small)


def iota(shape, dim):
    return lax.broadcasted_iota(jnp.int32, shape, dim)


def with_eye(rows):
    return rows + (iota(rows.shape, 0) == iota(rows.shape, 1)).astype(F32)


def spread(tile, column):
    lanes = iota(tile.shape, 1)
    return jnp.take_along_axis(tile, (lanes & ~(Q - 1)) + column, axis=1)


def invert_units(blocks):
    lanes, count = iota((8, H), 1), Q // 8
    strips, results = [], []
    for v in blocks:
        for i in range(count):
            strip = v[8 * i : 8 * i + 8]
            for k in range(1, H // Q):
                strip = jnp.where(lanes >= k * Q, v[k * Q + 8 * i : k * Q + 8 * i + 8], strip)
            strips.append(strip)
            results.append(((lanes & (Q - 1)) == iota((8, H), 0) + 8 * i).astype(F32))
    for j in range(Q - 1, 0, -1):
        for m in range(0, len(strips), count):
            row = results[m + j // 8][j % 8 : j % 8 + 1]
            for i in range((j - 1) // 8 + 1):
                column = spread(strips[m + i], j)
                if i == j // 8:
                    column = jnp.where(iota((8, H), 0) < j % 8, column, 0.0)
                results[m + i] = results[m + i] - column * row
    wide = iota((Q, H), 1)
    out = []
    for m in range(0, len(strips), count):
        packed = jnp.concatenate(results[m : m + count], axis=0)
        out.append(
            jnp.concatenate(
                [
                    jnp.where((wide >= k * Q) & (wide < (k + 1) * Q), packed, 0.0)
                    for k in range(H // Q)
                ],
                axis=0,
            )
        )
    span = Q
    while span < H:
        starts = range(0, H, 2 * span)

        def chosen(value):
            return jnp.concatenate([value[i : i + span] for i in starts], axis=0)

        def placed(value):
            gap, strips = jnp.zeros((span, H), F32), []
            for i in range(len(starts)):
                strips += [value[i * span : (i + 1) * span], gap]
            return jnp.concatenate(strips, axis=0)

        rows, cols = iota((H // 2, H), 0), iota((H // 2, H), 1)
        corner = ((cols & span) != 0) & (rows // span == cols // (2 * span))
        parts = [exact(jnp.where(corner, chosen(v), 0.0), t) for t, v in zip(out, blocks)]
        parts = [exact(chosen(t), placed(part)) for t, part in zip(out, parts)]
        out = [t - placed(part) for t, part in zip(out, parts)]
        span *= 2
    return out


def invert_unit_all(matrices):
    out = invert_units([v for v00, _, v11 in matrices for v in (v00, v11)])
    tops, bottoms = out[0::2], out[1::2]
    corners = [exact(v01, t11) for (_, v01, _), t11 in zip(matrices, bottoms)]
    corners = [-exact(t00, c) for t00, c in zip(tops, corners)]
    return list(zip(tops, corners, bottoms))


def scaled(parts):
    g00, g01, g11, d00, d11 = parts
    above = iota((H, H), 0) < iota((H, H), 1)
    eye = iota((H, H), 0) == iota((H, H), 1)
    r0, r1 = 2.0 / d00, 2.0 / d11
    unit = jnp.where(above, g00 * r0, 0.0), g01 * r1, jnp.where(above, g11 * r1, 0.0)
    scale = [jnp.sum(jnp.where(eye, r, 0.0), axis=1, keepdims=True) for r in (r0, r1)]
    return unit, scale


def solve(parts, p):
    (v00, v01, v11), (c0, c1) = scaled(parts)
    t00, t11 = invert_units([v00, v11])
    x1 = exact(t11, p[H:])
    x0 = exact(t00, p[:H] - exact(v01, x1))
    return jnp.concatenate([x0 * c0, x1 * c1], axis=0)


def inverses_of(grams):
    units, scales = zip(*[scaled(parts) for parts in grams])
    out = []
    for (t00, t01, t11), (c0, c1) in zip(invert_unit_all(units), scales):
        top = jnp.concatenate([t00 * c0, t01 * c0], axis=1)
        bottom = jnp.concatenate([jnp.zeros((H, H), F32), t11 * c1], axis=1)
        out.append(jnp.concatenate([top, bottom], axis=0))
    return out


def diagonal(block):
    eye = iota((H, H), 0) == iota((H, H), 1)
    return jnp.sum(jnp.where(eye, block, 0.0), axis=0, keepdims=True)


def full_parts(g):
    g00, g01, g11 = g[:H, :H], g[:H, H:], g[H:, H:]
    return g00, g01, g11, diagonal(g00), diagonal(g11)


def pack(g):
    keep = iota((H, H), 0) <= iota((H, H), 1)
    first = jnp.where(keep, g[:H, :H], g[H:, H:])
    diag = jnp.broadcast_to(diagonal(g[H:, H:]), (8, H))
    tail = jnp.concatenate([diag, jnp.zeros((8, H), F32)], axis=1)
    return jnp.concatenate([jnp.concatenate([first, g[:H, H:]], axis=1), tail], axis=0)


def packed_parts(m, live):
    first, d11 = m[:H, :H], m[H : H + 1, :H]
    one = jnp.where(live, 0.0, 1.0)
    return first, m[:H, H:], first.T, diagonal(first) + one, d11 + one


def panel(ref, s):
    return ref[:, :, s].reshape(2 * R, R)


def spread_kernel(value_ref, out_ref):
    for i in range(out_ref.shape[0]):
        out_ref[i] = value_ref[...]


def spread_parts_kernel(value_ref, *outs):
    start = 0
    for out_ref in outs:
        stop = start + out_ref.shape[2]
        for i in range(out_ref.shape[0]):
            out_ref[i] = value_ref[:, start:stop]
        start = stop


def in_middle():
    return lax.axis_index("xh") != lax.axis_index("core")


def store_by_core(core, low, up, c_ref, x_ref):
    @pl.when(core == 0)
    def _():
        c_ref[...] = low
        x_ref[...] = up

    @pl.when(core != 0)
    def _():
        c_ref[...] = up
        x_ref[...] = low


def first_kernel(g_ref, z_ref, out_ref, pc_ref, px_ref, c_ref, x_ref, a_ref):
    rows = panel(g_ref, 1)
    packed, turned = [], []
    for k, half in enumerate((rows[:R], with_eye(rows[R:]))):
        y, t = halves(half), halves(half.T)
        packed.append(pack(product(t, y)))
        turned.append(t)
        a_ref[k] = half
    y = with_eye(panel(g_ref, 0))
    yh, yt = halves(y), halves(y.T)
    z = z_ref[...]
    p = product(yt, halves(z))
    x = solve(full_parts(product(yt, yh)), p)
    z = z - product(yh, halves(x))
    out_ref[...] = z
    up = product(turned[0], halves(z[:R]))
    low = product(turned[1], halves(z[R:]))
    store_by_core(lax.axis_index("core"), low, up, pc_ref, px_ref)
    store_by_core(lax.axis_index("core"), packed[1], packed[0], c_ref, x_ref)


def second_kernel(g_ref, c_ref, c_in_ref, x_ref, x_in_ref, a_ref, mh_ref, ml_ref, nh_ref, nl_ref):
    y = with_eye(panel(g_ref, 0))
    turned = y.T
    t, tc, tx = inverses_of(
        [
            full_parts(product(halves(turned), halves(y))),
            packed_parts(c_ref[...] + c_in_ref[...], True),
            packed_parts(x_ref[...] + x_in_ref[...], in_middle()),
        ]
    )
    for i in range(0, 2 * R, H):
        mh_ref[:, i : i + H], ml_ref[:, i : i + H] = halves(exact(t, turned[:, i : i + H]))
    core = lax.axis_index("core")
    for k, half, inverse in ((0, 1 - core, tc), (1, core, tx)):
        for i in range(0, R, H):
            part = halves(exact(a_ref[half], inverse[:, i : i + H]))
            nh_ref[k, :, i : i + H], nl_ref[k, :, i : i + H] = part


def last_kernel(g_ref, z_ref, c_ref, c_in_ref, x_ref, x_in_ref, nh_ref, nl_ref, mh_ref, ml_ref, out_ref):
    core = lax.axis_index("core")
    pc = c_ref[...] + c_in_ref[...]
    px = x_ref[...] + x_in_ref[...]
    for k, half, p in ((0, 1 - core, pc), (1, core, px)):
        rows = pl.ds(pl.multiple_of(half * R, R), R)
        change = product((nh_ref[k], nl_ref[k]), halves(p))
        if k == 1:
            change = jnp.where(in_middle(), change, 0.0)
        out_ref[rows, :] = z_ref[rows, :] - change
    z = out_ref[...]
    x = product((mh_ref[...], ml_ref[...]), halves(z))
    out_ref[...] = z - product(halves(with_eye(panel(g_ref, 0))), halves(x))


VM = pl.BlockSpec(memory_space=pltpu.VMEM)
SM = pl.BlockSpec(memory_space=pltpu.SMEM)


def call(kernel, outs, args, flops, scalars=0):
    outs = [o if isinstance(o[0], tuple) else (o, F32) for o in outs]
    return pl.pallas_call(
        kernel,
        out_shape=[jax.ShapeDtypeStruct(s, d) for s, d in outs],
        in_specs=[SM] * scalars + [VM] * (len(args) - scalars),
        out_specs=[VM] * len(outs),
        cost_estimate=pl.CostEstimate(flops=flops, bytes_accessed=1 << 20, transcendentals=0),
        compiler_params=pltpu.CompilerParams(vmem_limit_bytes=12 << 20),
    )(*args)


def exchange(stack, axes):
    return lax.all_to_all(stack, axes, split_axis=0, concat_axis=0, tiled=True)


def swap_cores(value):
    return lax.ppermute(value, "core", [(0, 1), (1, 0)])


def swap_middle(value):
    return lax.ppermute(value, ("xh", "core"), [(1, 2), (2, 1)])


def local(eigen_rows, panels):
    (stack,) = call(spread_kernel, [(8, *panels.shape)], [panels], 10**6)
    near = exchange(stack, "z")
    early, late = call(
        spread_parts_kernel, [(8, 8, 2, 8, R), (8, 8, 1, 8, R)], [near], 10**6
    )
    every = exchange(early, ("y", "xl"))
    third = exchange(late, ("y", "xl"))
    columns = eigen_rows.shape[1]
    half = ((2, R, R), BF16)
    big = 10**9
    z, pc, px, c, x, a = call(
        first_kernel,
        [eigen_rows.shape, (R, columns), (R, columns)] + [(H + 8, R)] * 2 + [(2, R, R)],
        [every, eigen_rows],
        8 * big,
    )
    x_in, c_in = swap_middle(x), swap_cores(c)
    px_in, pc_in = swap_middle(px), swap_cores(pc)
    mh, ml, nh, nl = call(
        second_kernel,
        [((R, 2 * R), BF16)] * 2 + [half] * 2,
        [third, c, c_in, x, x_in, a],
        8 * big,
    )
    (out,) = call(
        last_kernel,
        [eigen_rows.shape],
        [third, z, pc, pc_in, px, px_in, nh, nl, mh, ml],
        2 * big,
    )
    return out


def solution(mesh):
    fine = Mesh(mesh.devices.reshape(2, 2, 4, 2, 8), ("xh", "core", "y", "xl", "z"))
    slab = P(("xh", "core"), ("y", "xl", "z"))
    strips = P(None, ("xh", "core", "y", "xl", "z"), None)
    return jax.shard_map(local, mesh=fine, in_specs=(slab, strips), out_specs=slab, check_vma=False)
```
